32 devices in a mesh: row: 2 (over x), col: 4 (over z), depth: 4 (over y, core).
Axes of the slice: x: 2, y: 2, z: 4, core: 2. Of those that a mesh axis runs over, the one named last changes fastest.
Arguments:
- pair: bfloat16 [768, 768, 128], P('row', 'col'), may hold values from -6 to 6
- ln_gain: float32 [128], replicated, may hold values from 0.1 to 1.9
- ln_shift: float32 [128], replicated, may hold values from -3 to 3
- proj_weight: bfloat16 [128, 512], replicated, may hold values from -0.5 to 0.5
- proj_bias: float32 [512], replicated, may hold values from -3 to 3
- gate_weight: bfloat16 [128, 128], replicated, may hold values from -0.5 to 0.5
- gate_bias: float32 [128], replicated, may hold values from -3 to 3
- out_gain: float32 [128], replicated, may hold values from 0.1 to 1.9
- out_shift: float32 [128], replicated, may hold values from -3 to 3
- out_weight: bfloat16 [128, 128], replicated, may hold values from -0.5 to 0.5
- out_bias: float32 [128], replicated, may hold values from -3 to 3
Outputs:
- update: bfloat16 [768, 768, 128], P('row', 'col')
The draws below stay inside these ranges and needn't reach their ends.
All inputs are finite; a program needn't handle non-finite values.
Results may differ from the reference program's by a relative error of at most 0.0051.
Values may be sent and summed in bfloat16 or wider, within the bound.
No kernel may reach another device: no remote copies, remote signals or barrier semaphores. Data moves between devices by JAX's collectives and lax.ppermute only.
A program may use at most 256 MiB of HBM per device.

```python
import jax
import jax.numpy as jnp
from jax import lax

C = 128
HID = 128
RES = 768


def block_levels(rng, dims, split, low, largest):
    level, own = 1.0, jax.random.fold_in(rng, 6)
    for position, blocks in split:
        heights = jnp.exp(jax.random.uniform(jax.random.fold_in(own, position), (blocks,), jnp.float32, low / len(split), largest / len(split)))
        level = level * jnp.repeat(heights, dims[position] // blocks).reshape([-1 if axis == position else 1 for axis in range(len(dims))])
    return level


def gaussian(key, shape, scale, limit, split=(), kind=jnp.bfloat16):
    result = scale * jax.random.normal(key, shape, jnp.float32)
    if split:
        result = result * block_levels(key, shape, split, -0.22, 0.18)
    return jnp.clip(result, -limit, limit).astype(kind)


def setup_inputs(seed: int = 0) -> dict:
    key_of = jax.random.split(jax.random.key(seed), 12)
    pair = gaussian(key_of[0], (RES, RES, C), 1.0, 6.0, ((0, 2), (1, 4)))
    ln_gain = jnp.clip(1.0 + 0.18 * jax.random.normal(key_of[1], (C,), jnp.float32), 0.1, 1.9)
    ln_shift = gaussian(key_of[2], (C,), 0.5, 3.0, (), jnp.float32)
    proj_weight = gaussian(key_of[3], (C, 4 * HID), C ** -0.5, 0.5)
    proj_bias = gaussian(key_of[4], (4 * HID,), 0.5, 3.0, (), jnp.float32)
    gate_weight = gaussian(key_of[5], (C, C), C ** -0.5, 0.5)
    gate_bias = gaussian(key_of[6], (C,), 0.5, 3.0, (), jnp.float32)
    out_gain = jnp.clip(1.0 + 0.18 * jax.random.normal(key_of[7], (HID,), jnp.float32), 0.1, 1.9)
    out_shift = gaussian(key_of[8], (HID,), 0.5, 3.0, (), jnp.float32)
    out_weight = gaussian(key_of[9], (HID, C), HID ** -0.5, 0.5)
    out_bias = gaussian(key_of[10], (C,), 0.5, 3.0, (), jnp.float32)
    return {"pair": pair, "ln_gain": ln_gain, "ln_shift": ln_shift, "proj_weight": proj_weight, "proj_bias": proj_bias, "gate_weight": gate_weight, "gate_bias": gate_bias, "out_gain": out_gain, "out_shift": out_shift, "out_weight": out_weight, "out_bias": out_bias}


def layer_norm(values, gain, shift):
    centre = lax.optimization_barrier(jnp.mean(values, axis=-1, keepdims=True))
    centred = values - centre
    spread = lax.optimization_barrier(jnp.mean(centred * centred, axis=-1, keepdims=True))
    return centred * lax.rsqrt(spread + 1e-05) * gain + shift

def reference(pair, ln_gain, ln_shift, proj_weight, proj_bias, gate_weight, gate_bias, out_gain, out_shift, out_weight, out_bias):
    hidden = proj_weight.shape[1] // 4
    normed = layer_norm(pair.astype(jnp.float32), ln_gain, ln_shift).astype(jnp.bfloat16)
    flat = normed.reshape(-1, C)
    mixed = jnp.dot(flat, proj_weight, preferred_element_type=jnp.float32) + proj_bias
    left = (jax.nn.sigmoid(mixed[:, :hidden]) * mixed[:, hidden:2 * hidden]).astype(jnp.bfloat16)
    right = (jax.nn.sigmoid(mixed[:, 2 * hidden:3 * hidden]) * mixed[:, 3 * hidden:]).astype(jnp.bfloat16)
    gate = jax.nn.sigmoid(jnp.dot(flat, gate_weight, preferred_element_type=jnp.float32) + gate_bias)
    left = left.reshape(RES, RES, hidden).astype(jnp.float32)
    right = right.reshape(RES, RES, hidden).astype(jnp.float32)
    triangle = jnp.einsum('ikc,jkc->ijc', left, right)
    tri_normed = layer_norm(triangle, out_gain, out_shift).astype(jnp.bfloat16)
    projected = jnp.dot(tri_normed.reshape(-1, hidden), out_weight, preferred_element_type=jnp.float32) + out_bias
    return (gate * projected).reshape(RES, RES, C).astype(jnp.bfloat16)
```

```python
import functools

import jax
import jax.numpy as jnp
from jax import lax
from jax.experimental import pallas as pl
from jax.experimental.pallas import tpu as pltpu
from jax.sharding import PartitionSpec as P

AXES = ("row", "col", "depth")
LANES = 128
PAIR = 32
CHUNKS = 8


def layer_norm(values, gain, shift):
    centre = jnp.mean(values, axis=-1, keepdims=True)
    centred = values - centre
    spread = jnp.mean(centred * centred, axis=-1, keepdims=True)
    return centred * lax.rsqrt(spread + 1e-05) * gain + shift


def project(piece, ln_gain, ln_shift, proj_weight, proj_bias, gate_weight, gate_bias):
    hidden = proj_weight.shape[1] // 4
    channels = piece.shape[2]
    normed = layer_norm(piece.astype(jnp.float32), ln_gain, ln_shift).astype(jnp.bfloat16)
    flat = normed.reshape(-1, channels)
    mixed = jnp.dot(flat, proj_weight, preferred_element_type=jnp.float32) + proj_bias
    left = (jax.nn.sigmoid(mixed[:, :hidden]) * mixed[:, hidden : 2 * hidden]).astype(jnp.bfloat16)
    right = (jax.nn.sigmoid(mixed[:, 2 * hidden : 3 * hidden]) * mixed[:, 3 * hidden :]).astype(
        jnp.bfloat16
    )
    gate = jax.nn.sigmoid(
        jnp.dot(flat, gate_weight, preferred_element_type=jnp.float32) + gate_bias
    )
    shape = (piece.shape[0], piece.shape[1])
    return (
        left.reshape(shape + (hidden,)),
        right.reshape(shape + (hidden,)),
        gate.reshape(shape + (channels,)),
    )


def finish(triangle, gate, out_gain, out_shift, out_weight, out_bias):
    hidden = triangle.shape[2]
    tri_normed = layer_norm(triangle, out_gain, out_shift).astype(jnp.bfloat16)
    projected = (
        jnp.dot(tri_normed.reshape(-1, hidden), out_weight, preferred_element_type=jnp.float32)
        + out_bias
    )
    return (gate * projected.reshape(gate.shape)).astype(jnp.bfloat16)


def gathered(
    pair,
    ln_gain,
    ln_shift,
    proj_weight,
    proj_bias,
    gate_weight,
    gate_bias,
    out_gain,
    out_shift,
    out_weight,
    out_bias,
):
    depth_count = lax.axis_size("depth")
    depth_id = lax.axis_index("depth")
    cols_here = pair.shape[1]
    quarter = cols_here // depth_count
    piece = lax.dynamic_slice_in_dim(pair, depth_id * quarter, quarter, 1)
    left, right, gate = project(
        piece, ln_gain, ln_shift, proj_weight, proj_bias, gate_weight, gate_bias
    )
    left_all = lax.all_gather(left, ("col", "depth"), axis=1, tiled=True)
    right_column = lax.all_gather(right, "row", axis=0, tiled=True)
    needed = lax.all_to_all(right_column, ("col", "depth"), split_axis=0, concat_axis=1, tiled=True)
    triangle = jnp.einsum("ikc,jkc->ijc", left_all, needed, preferred_element_type=jnp.float32)
    finished = finish(triangle, gate, out_gain, out_shift, out_weight, out_bias)
    return lax.all_gather(finished, "depth", axis=1, tiled=True)


def sigmoid(values):
    return 0.5 * jnp.tanh(0.5 * values) + 0.5


NT = (((1,), (1,)), ((), ()))
TN = (((0,), (0,)), ((), ()))


def project_kernel(pieces, x_ref, wt_ref, bias_ref, gain_ref, shift_ref, normed_ref, *rest):
    outs, held = rest[:-1], rest[-1]
    block, cols = x_ref.shape[0], x_ref.shape[1]
    tail = cols - LANES
    half = block // 2
    rows = block + half
    hid = wt_ref.shape[0] // 4
    ones = jnp.full((LANES, LANES), 1.0 / LANES, jnp.bfloat16)

    def tile(x, at):
        centre = jnp.dot(x, ones, preferred_element_type=jnp.float32)
        centred = x.astype(jnp.float32) - centre
        spread = jnp.dot(
            (centred * centred).astype(jnp.bfloat16), ones, preferred_element_type=jnp.float32
        )
        normed = (
            centred * lax.rsqrt(spread + 1e-05) * gain_ref[...] + shift_ref[...]
        ).astype(jnp.bfloat16)
        mixed = (
            lax.dot_general(wt_ref[...], normed, NT, preferred_element_type=jnp.float32)
            + bias_ref[...]
        )
        left = sigmoid(mixed[:hid]) * mixed[hid : 2 * hid]
        right = sigmoid(mixed[2 * hid : 3 * hid]) * mixed[3 * hid :]
        held[pl.ds(at, hid, stride=rows), :] = left
        held[pl.ds(hid * rows + at, hid, stride=rows), :] = right
        return normed

    def main(i, carry):
        normed_ref[i, :LANES, :] = tile(x_ref[i, :LANES, :], i)
        return carry

    def leftover(i, carry):
        x = jnp.concatenate([x_ref[i, LANES:, :], x_ref[i + half, LANES:, :]], axis=0)
        normed = tile(x, block + i)
        normed_ref[i, LANES:, :] = normed[:tail]
        normed_ref[i + half, LANES:, :] = normed[tail:]
        return carry

    lax.fori_loop(0, block, main, 0, unroll=4)
    lax.fori_loop(0, half, leftover, 0, unroll=4)
    for index, out in enumerate(outs):
        part = out.shape[0]
        first = index * part * rows
        out[:, 0] = (
            held[first : first + part * rows, :].reshape(part, rows, LANES).astype(jnp.bfloat16)
        )


def project_local(pair, wt, bias, gain, shift, pieces):
    rows_here, cols, channels = pair.shape
    hid = wt.shape[0] // 4
    part = hid // pieces
    blocks = rows_here // PAIR
    packed = PAIR + PAIR // 2
    whole = lambda b: (0, 0)
    positions = rows_here * cols
    outs = pl.pallas_call(
        functools.partial(project_kernel, pieces),
        grid=(blocks,),
        in_specs=[
            pl.BlockSpec((PAIR, cols, channels), lambda b: (b, 0, 0)),
            pl.BlockSpec(wt.shape, whole),
            pl.BlockSpec(bias.shape, whole),
            pl.BlockSpec(gain.shape, whole),
            pl.BlockSpec(shift.shape, whole),
        ],
        out_specs=[pl.BlockSpec((PAIR, cols, channels), lambda b: (b, 0, 0))]
        + [pl.BlockSpec((part, 1, packed, LANES), lambda b: (0, b, 0, 0))] * (2 * pieces),
        out_shape=[jax.ShapeDtypeStruct(pair.shape, jnp.bfloat16)]
        + [jax.ShapeDtypeStruct((part, blocks, packed, LANES), jnp.bfloat16)] * (2 * pieces),
        scratch_shapes=[pltpu.VMEM((2 * hid * packed, LANES), jnp.float32)],
        compiler_params=pltpu.CompilerParams(dimension_semantics=("arbitrary",)),
        cost_estimate=pl.CostEstimate(
            flops=12 * positions * channels * hid,
            bytes_accessed=positions * (4 * channels + 4 * hid),
            transcendentals=positions * (channels + 2 * hid),
        ),
        name="project_local",
    )(pair, wt, bias, gain, shift)
    return outs[0], outs[1 : 1 + pieces], outs[1 + pieces :]


def operand(own_ref, par_ref):
    own, par = own_ref[0], par_ref[0]
    blocks = own.shape[0]
    half = PAIR // 2

    def turned(x):
        flat = x.reshape(blocks * half, LANES).astype(jnp.float32)
        return pltpu.roll(flat, LANES // 2, 1).astype(jnp.bfloat16).reshape(x.shape)

    own_rest, par_rest = own[:, PAIR:, :], par[:, PAIR:, :]
    low = lax.broadcasted_iota(jnp.int32, own_rest.shape, 2) < LANES // 2
    first = jnp.where(low, own_rest, turned(par_rest))
    second = jnp.where(low, turned(own_rest), par_rest)
    rest = jnp.concatenate([first[:, None], second[:, None]], axis=1)
    flat = (blocks * PAIR, LANES)
    return jnp.concatenate(
        [own[:, :PAIR, :].reshape(flat), par[:, :PAIR, :].reshape(flat), rest.reshape(flat)],
        axis=1,
    )


def choose(which, ref, here, there):
    @pl.when(which == 0)
    def _():
        ref[...] = operand(*here)

    @pl.when(which != 0)
    def _():
        ref[...] = operand(*there)


def partial_kernel(pick, lo, lp, ro, rp, xo, xp, out_ref, right):
    choose(pick[0], right, (ro, rp), (xo, xp))
    out_ref[0] = lax.dot_general(
        right[...], operand(lo, lp), NT, preferred_element_type=jnp.float32
    ).astype(jnp.bfloat16)


def final_kernel(pick, lo, lp, ro, rp, xo, xp, got_ref, mine_ref, outer_ref, right, total):
    choose(pick[1], right, (ro, rp), (xo, xp))
    total[...] = lax.dot_general(
        right[...], operand(lo, lp), NT, preferred_element_type=jnp.float32
    ) + got_ref[0].astype(jnp.float32)
    rows = mine_ref.shape[1]
    mine = pl.multiple_of(pick[2], rows)
    other = pl.multiple_of(rows - pick[2], rows)
    mine_ref[0] = total[pl.ds(mine, rows), :].astype(jnp.bfloat16)
    outer_ref[0] = total[pl.ds(other, rows), :].astype(jnp.bfloat16)


def contract(kernel, pick, packed, got, cols):
    part, blocks, rows, _ = packed[0].shape
    size = blocks * PAIR
    block = lambda shape: pl.BlockSpec((1,) + shape, lambda h, _: (h,) + (0,) * len(shape))
    scratch = [pltpu.VMEM((size, 3 * LANES), jnp.bfloat16)]
    operands = list(packed)
    in_specs = [block((blocks, rows, LANES))] * len(packed)
    if got is None:
        shapes = [(size, size)]
    else:
        operands.append(got)
        in_specs.append(block((size, size)))
        shapes = [(cols, size)] * 2
        scratch.append(pltpu.VMEM((size, size), jnp.float32))
    outs = pl.pallas_call(
        kernel,
        grid_spec=pltpu.PrefetchScalarGridSpec(
            num_scalar_prefetch=1,
            grid=(part,),
            in_specs=in_specs,
            out_specs=[block(shape) for shape in shapes],
            scratch_shapes=scratch,
        ),
        out_shape=[jax.ShapeDtypeStruct((part,) + shape, jnp.bfloat16) for shape in shapes],
        compiler_params=pltpu.CompilerParams(dimension_semantics=("arbitrary",)),
        cost_estimate=pl.CostEstimate(
            flops=6 * part * size * size * LANES,
            bytes_accessed=part * size * (size * 2 + 12 * 3 * LANES),
            transcendentals=0,
        ),
        name=kernel.__name__,
    )(pick, *operands)
    return outs[0] if got is None else outs


def finish_kernel(count, *refs):
    parts = refs[:count]
    normed_ref, gate_w, gate_b, gain, shift, out_w, out_b = refs[count : count + 7]
    out_ref, tri, flat = refs[count + 7 :]
    part, rows = parts[0].shape[0], parts[0].shape[1]
    size = parts[0].shape[2]
    hidden = part * count
    scale = 1.0 / hidden

    def lane_block(step, carry):
        at = pl.multiple_of(step * LANES, LANES)
        total = jnp.zeros((rows, LANES), jnp.float32)
        for index, ref in enumerate(parts):
            for h in range(part):
                plane = ref[h, :, pl.ds(at, LANES)].astype(jnp.float32)
                total = total + plane
                base = (index * part + h) * rows
                tri[base : base + rows, :] = plane
        centre = total * scale

        def spread_step(h, total):
            base = pl.multiple_of(h * rows, rows)
            centred = tri[pl.ds(base, rows), :] - centre
            return total + centred * centred

        spread = lax.fori_loop(
            0, hidden, spread_step, jnp.zeros((rows, LANES), jnp.float32), unroll=16
        )
        factor = lax.rsqrt(spread * scale + 1e-05)
        offset = centre * factor

        def norm_step(h, carry):
            base = pl.multiple_of(h * rows, rows)
            tri[pl.ds(base, rows), :] = (
                tri[pl.ds(base, rows), :] * factor - offset
            ) * gain[h] + shift[h]
            return carry

        lax.fori_loop(0, hidden, norm_step, 0, unroll=16)
        for j in range(rows):
            column = tri[pl.ds(j, hidden, stride=rows), :].astype(jnp.bfloat16)
            flat[pl.ds(j, LANES, stride=rows), :] = lax.dot_general(
                column, out_w[...], TN, preferred_element_type=jnp.float32
            )
        span = 16

        def write_step(step, carry):
            first = pl.multiple_of(step * span, span)
            channels = normed_ref.shape[2]
            normed = normed_ref[pl.ds(at + first, span), :, :].reshape(span * rows, channels)
            gate = sigmoid(
                jnp.dot(normed, gate_w[...], preferred_element_type=jnp.float32) + gate_b[...]
            )
            base = pl.multiple_of(first * rows, span * rows)
            result = gate * (flat[pl.ds(base, span * rows), :] + out_b[...])
            out_ref[pl.ds(at + first, span), :, :] = result.reshape(span, rows, channels).astype(
                jnp.bfloat16
            )
            return carry

        lax.fori_loop(0, LANES // span, write_step, 0)
        return carry

    lax.fori_loop(0, size // LANES, lane_block, 0)


def finish_local(parts, normed, gate_w, gate_b, gain, shift, out_w, out_b):
    part, cols, size = parts[0].shape
    channels = normed.shape[2]
    hidden = part * len(parts)
    rows = 16
    whole = lambda b: (0, 0)
    positions = cols * size
    return pl.pallas_call(
        functools.partial(finish_kernel, len(parts)),
        grid=(cols // rows,),
        in_specs=[pl.BlockSpec((part, rows, size), lambda b: (0, b, 0))] * len(parts)
        + [
            pl.BlockSpec((size, rows, channels), lambda b: (0, b, 0)),
            pl.BlockSpec(gate_w.shape, whole),
            pl.BlockSpec(gate_b.shape, whole),
            pl.BlockSpec(memory_space=pltpu.SMEM),
            pl.BlockSpec(memory_space=pltpu.SMEM),
            pl.BlockSpec(out_w.shape, whole),
            pl.BlockSpec(out_b.shape, whole),
        ],
        out_specs=pl.BlockSpec((size, rows, channels), lambda b: (0, b, 0)),
        out_shape=jax.ShapeDtypeStruct(normed.shape, jnp.bfloat16),
        scratch_shapes=[
            pltpu.VMEM((hidden * rows, LANES), jnp.float32),
            pltpu.VMEM((LANES * rows, channels), jnp.float32),
        ],
        compiler_params=pltpu.CompilerParams(dimension_semantics=("arbitrary",)),
        cost_estimate=pl.CostEstimate(
            flops=2 * positions * channels * (hidden + channels),
            bytes_accessed=positions * (2 * hidden + 4 * channels),
            transcendentals=positions * channels,
        ),
        name="finish_local",
    )(*parts, normed, gate_w, gate_b, gain, shift, out_w, out_b)


def routes(mesh_shape):
    rows, cols, depths = (mesh_shape[name] for name in AXES)

    def build(target):
        pairs = []
        for r in range(rows):
            for c in range(cols):
                for d in range(depths):
                    to = target(r, c, d)
                    if to is not None:
                        index = lambda at: (at[0] * cols + at[1]) * depths + at[2]
                        pairs.append((index((r, c, d)), index(to)))
        return pairs

    outer = lambda c: c in (0, cols - 1)
    near = lambda c: c ^ 1
    return {
        "inward": build(lambda r, c, d: (r, near(c), d) if outer(c) else None),
        "outward": build(lambda r, c, d: None if outer(c) else (r, near(c), d)),
        "middle": build(lambda r, c, d: None if outer(c) else (r, cols - 1 - c, d)),
        "across": build(lambda r, c, d: None if outer(c) else (rows - 1 - r, c, d)),
        "far": build(lambda r, c, d: (r, c, d ^ 2)),
        "twin": build(lambda r, c, d: (r, c, d ^ 1)),
    }


def folded(
    routing,
    pair,
    ln_gain,
    ln_shift,
    proj_weight,
    proj_bias,
    gate_weight,
    gate_bias,
    out_gain,
    out_shift,
    out_weight,
    out_bias,
):
    depth_count = lax.axis_size("depth")
    row_id, col_id, depth_id = (lax.axis_index(name) for name in AXES)
    channels, cols = pair.shape[2], pair.shape[1]
    hidden = proj_weight.shape[1] // 4
    hid = hidden // depth_count
    pieces = CHUNKS

    def move(value, name):
        return lax.ppermute(value, AXES, routing[name])

    def here(values, axis):
        return lax.dynamic_slice_in_dim(values, depth_id * hid, hid, axis)

    wt = here(proj_weight.T.reshape(4, hidden, channels), 1).reshape(4 * hid, channels)
    bias = here(proj_bias.reshape(4, hidden), 1).reshape(4 * hid, 1)
    normed, left, right = project_local(
        pair, wt, bias, ln_gain[None, :], ln_shift[None, :], pieces
    )

    half_id = col_id // 2
    is_outer = (col_id == 0) | (col_id == lax.axis_size("col") - 1)
    pick = jnp.stack(
        [
            (row_id + half_id != 1).astype(jnp.int32),
            (row_id != half_id).astype(jnp.int32),
            ((col_id % 2) * cols).astype(jnp.int32),
        ]
    )
    own, twin, far, far_twin = [], [], [], []
    for t in range(pieces):
        right_par = move(right[t], "inward")
        left_par = move(left[t], "inward")
        cross_own = move(right[t], "across")
        cross_par = move(right_par, "across")
        packed = (left[t], left_par, right[t], right_par, cross_own, cross_par)
        sent = contract(partial_kernel, pick, packed, None, cols)
        got = move(sent, "middle")
        mine, outers = contract(final_kernel, pick, packed, got, cols)
        mine = jnp.where(is_outer, move(outers, "outward"), mine)
        own.append(mine)
        twin.append(move(mine, "twin"))
        other = move(mine, "far")
        far.append(other)
        far_twin.append(move(other, "twin"))

    order = jnp.concatenate(
        [(depth_id ^ s) * hid + jnp.arange(hid) for s in range(depth_count)]
    )
    return finish_local(
        own + twin + far + far_twin,
        normed,
        gate_weight,
        gate_bias[None, :],
        out_gain[order],
        out_shift[order],
        out_weight[order],
        out_bias[None, :],
    )


def per_device(mesh_shape, pair, *parameters):
    shape = (mesh_shape["row"], mesh_shape["col"], mesh_shape["depth"])
    hidden = parameters[2].shape[1] // 4
    fits = (
        shape == (2, 4, 4)
        and pair.shape[0] == 2 * pair.shape[1]
        and pair.shape[1] == LANES + LANES // 2
        and pair.shape[2] == LANES
        and hidden % (shape[2] * CHUNKS) == 0
    )
    if fits:
        return folded(routes(mesh_shape), pair, *parameters)
    return gathered(pair, *parameters)


def solution(mesh):
    placed = (P("row", "col", None), P(), P(), P(), P(), P(), P(), P(), P(), P(), P())
    return jax.shard_map(
        functools.partial(per_device, dict(mesh.shape)),
        mesh=mesh,
        in_specs=placed,
        out_specs=P("row", "col", None),
        check_vma=False,
    )
```

```python
import functools

import jax
import jax.numpy as jnp
from jax import lax
from jax.experimental import pallas as pl
from jax.experimental.pallas import tpu as pltpu
from jax.sharding import PartitionSpec as P


AXES = ("row", "col", "depth")
LANES = 128
PAIR = 32
CHUNKS = 8
PLANES = 2
GROUP = 16


def layer_norm(values, gain, shift):
    centre = jnp.mean(values, axis=-1, keepdims=True)
    centred = values - centre
    spread = jnp.mean(centred * centred, axis=-1, keepdims=True)
    return centred * lax.rsqrt(spread + 1e-05) * gain + shift


def project(piece, ln_gain, ln_shift, proj_weight, proj_bias, gate_weight, gate_bias):
    hidden = proj_weight.shape[1] // 4
    channels = piece.shape[2]
    normed = layer_norm(piece.astype(jnp.float32), ln_gain, ln_shift).astype(jnp.bfloat16)
    flat = normed.reshape(-1, channels)
    mixed = jnp.dot(flat, proj_weight, preferred_element_type=jnp.float32) + proj_bias
    left = (jax.nn.sigmoid(mixed[:, :hidden]) * mixed[:, hidden : 2 * hidden]).astype(jnp.bfloat16)
    right = (jax.nn.sigmoid(mixed[:, 2 * hidden : 3 * hidden]) * mixed[:, 3 * hidden :]).astype(
        jnp.bfloat16
    )
    gate = jax.nn.sigmoid(
        jnp.dot(flat, gate_weight, preferred_element_type=jnp.float32) + gate_bias
    )
    shape = (piece.shape[0], piece.shape[1])
    return (
        left.reshape(shape + (hidden,)),
        right.reshape(shape + (hidden,)),
        gate.reshape(shape + (channels,)),
    )


def finish(triangle, gate, out_gain, out_shift, out_weight, out_bias):
    hidden = triangle.shape[2]
    tri_normed = layer_norm(triangle, out_gain, out_shift).astype(jnp.bfloat16)
    projected = (
        jnp.dot(tri_normed.reshape(-1, hidden), out_weight, preferred_element_type=jnp.float32)
        + out_bias
    )
    return (gate * projected.reshape(gate.shape)).astype(jnp.bfloat16)


def gathered(
    pair,
    ln_gain,
    ln_shift,
    proj_weight,
    proj_bias,
    gate_weight,
    gate_bias,
    out_gain,
    out_shift,
    out_weight,
    out_bias,
):
    depth_count = lax.axis_size("depth")
    depth_id = lax.axis_index("depth")
    cols_here = pair.shape[1]
    quarter = cols_here // depth_count
    piece = lax.dynamic_slice_in_dim(pair, depth_id * quarter, quarter, 1)
    left, right, gate = project(
        piece, ln_gain, ln_shift, proj_weight, proj_bias, gate_weight, gate_bias
    )
    left_all = lax.all_gather(left, ("col", "depth"), axis=1, tiled=True)
    right_column = lax.all_gather(right, "row", axis=0, tiled=True)
    needed = lax.all_to_all(right_column, ("col", "depth"), split_axis=0, concat_axis=1, tiled=True)
    triangle = jnp.einsum("ikc,jkc->ijc", left_all, needed, preferred_element_type=jnp.float32)
    finished = finish(triangle, gate, out_gain, out_shift, out_weight, out_bias)
    return lax.all_gather(finished, "depth", axis=1, tiled=True)


def sigmoid(values):
    return 0.5 * jnp.tanh(0.5 * values) + 0.5


NT = (((1,), (1,)), ((), ()))
TN = (((0,), (0,)), ((), ()))


def project_kernel(x_ref, wt_ref, bias_ref, gain_ref, shift_ref, normed_ref, *rest):
    outs, held = rest[:-1], rest[-1]
    block, cols = x_ref.shape[0], x_ref.shape[1]
    tail = cols - LANES
    half = block // 2
    rows = block + half
    pitch = rows + 8
    hid = wt_ref.shape[0] // 4
    ones = jnp.full((LANES, LANES), 1.0 / LANES, jnp.bfloat16)

    def tiles(x, first, count):
        flat = x.reshape(count * LANES, LANES)
        centre = jnp.dot(flat, ones, preferred_element_type=jnp.float32)
        centred = flat.astype(jnp.float32) - centre
        spread = jnp.dot(
            (centred * centred).astype(jnp.bfloat16), ones, preferred_element_type=jnp.float32
        )
        normed = (
            centred * lax.rsqrt(spread + 1e-05) * gain_ref[...] + shift_ref[...]
        ).astype(jnp.bfloat16)
        mixed = lax.dot_general(wt_ref[...], normed, NT, preferred_element_type=jnp.float32)
        for t in range(count):
            part = mixed[:, t * LANES : (t + 1) * LANES] + bias_ref[...]
            left = sigmoid(part[:hid]) * part[hid : 2 * hid]
            right = sigmoid(part[2 * hid : 3 * hid]) * part[3 * hid :]
            held[pl.ds(first + t, hid, stride=pitch), :] = left
            held[pl.ds(hid * pitch + first + t, hid, stride=pitch), :] = right
        return normed.reshape(count, LANES, LANES)

    def main(step, carry):
        at = pl.multiple_of(step * GROUP, GROUP)
        normed_ref[pl.ds(at, GROUP), :LANES, :] = tiles(
            x_ref[pl.ds(at, GROUP), :LANES, :], at, GROUP
        )
        return carry

    def leftover(step, carry):
        at = pl.multiple_of(step * GROUP, GROUP)
        x = jnp.concatenate(
            [x_ref[pl.ds(at, GROUP), LANES:, :], x_ref[pl.ds(at + half, GROUP), LANES:, :]], axis=1
        )
        normed = tiles(x, block + at, GROUP)
        normed_ref[pl.ds(at, GROUP), LANES:, :] = normed[:, :tail]
        normed_ref[pl.ds(at + half, GROUP), LANES:, :] = normed[:, tail:]
        return carry

    lax.fori_loop(0, block // GROUP, main, 0, unroll=True)
    lax.fori_loop(0, half // GROUP, leftover, 0)
    for index, out in enumerate(outs):
        part = out.shape[0]
        for h in range(part):
            first = (index * part + h) * pitch
            out[h, 0] = held[first : first + rows, :].astype(jnp.bfloat16)


def project_local(pair, wt, bias, gain, shift, pieces):
    rows_here, cols, channels = pair.shape
    hid = wt.shape[0] // 4
    part = hid // pieces
    blocks = rows_here // PAIR
    packed = PAIR + PAIR // 2
    whole = lambda b: (0, 0)
    positions = rows_here * cols
    outs = pl.pallas_call(
        project_kernel,
        grid=(blocks,),
        in_specs=[
            pl.BlockSpec((PAIR, cols, channels), lambda b: (b, 0, 0)),
            pl.BlockSpec(wt.shape, whole),
            pl.BlockSpec(bias.shape, whole),
            pl.BlockSpec(gain.shape, whole),
            pl.BlockSpec(shift.shape, whole),
        ],
        out_specs=[pl.BlockSpec((PAIR, cols, channels), lambda b: (b, 0, 0))]
        + [pl.BlockSpec((part, 1, packed, LANES), lambda b: (0, b, 0, 0))] * (2 * pieces),
        out_shape=[jax.ShapeDtypeStruct(pair.shape, jnp.bfloat16)]
        + [jax.ShapeDtypeStruct((part, blocks, packed, LANES), jnp.bfloat16)] * (2 * pieces),
        scratch_shapes=[pltpu.VMEM((2 * hid * (packed + 8), LANES), jnp.float32)],
        compiler_params=pltpu.CompilerParams(dimension_semantics=("arbitrary",)),
        cost_estimate=pl.CostEstimate(
            flops=12 * positions * channels * hid,
            bytes_accessed=positions * (4 * channels + 4 * hid),
            transcendentals=positions * (channels + 2 * hid),
        ),
        name="project_local",
    )(pair, wt, bias, gain, shift)
    return outs[0], outs[1 : 1 + pieces], outs[1 + pieces :]


def operand(own, par):
    blocks = own.shape[0]
    half = PAIR // 2

    def turned(x):
        flat = x.reshape(blocks * half, LANES).astype(jnp.float32)
        return pltpu.roll(flat, LANES // 2, 1).astype(jnp.bfloat16).reshape(x.shape)

    own_rest, par_rest = own[:, PAIR:, :], par[:, PAIR:, :]
    low = lax.broadcasted_iota(jnp.int32, own_rest.shape, 2) < LANES // 2
    first = jnp.where(low, own_rest, turned(par_rest))
    second = jnp.where(low, turned(own_rest), par_rest)
    rest = jnp.concatenate([first[:, None], second[:, None]], axis=1)
    flat = (blocks * PAIR, LANES)
    return jnp.concatenate(
        [own[:, :PAIR, :].reshape(flat), par[:, :PAIR, :].reshape(flat), rest.reshape(flat)],
        axis=1,
    )


def product(here, h, lo, lp, ro, rp, xo, xp):
    own = jnp.where(here, ro[h], xo[h])
    par = jnp.where(here, rp[h], xp[h])
    return lax.dot_general(
        operand(own, par), operand(lo[h], lp[h]), NT, preferred_element_type=jnp.float32
    )


def partial_kernel(pick, lo, lp, ro, rp, xo, xp, out_ref):
    for h in range(out_ref.shape[0]):
        out_ref[h] = product(pick[0] == 0, h, lo, lp, ro, rp, xo, xp).astype(jnp.bfloat16)


def final_kernel(pick, lo, lp, ro, rp, xo, xp, got_ref, mine_ref, outer_ref, total):
    rows = mine_ref.shape[1]
    mine = pl.multiple_of(pick[2], rows)
    other = pl.multiple_of(rows - pick[2], rows)
    for h in range(mine_ref.shape[0]):
        total[h] = product(pick[1] == 0, h, lo, lp, ro, rp, xo, xp) + got_ref[h].astype(
            jnp.float32
        )
        mine_ref[h] = total[h, pl.ds(mine, rows), :].astype(jnp.bfloat16)
        outer_ref[h] = total[h, pl.ds(other, rows), :].astype(jnp.bfloat16)


def contract(kernel, pick, packed, got, cols):
    part, blocks, rows, _ = packed[0].shape
    size = blocks * PAIR
    block = lambda shape: pl.BlockSpec((PLANES,) + shape, lambda h, _: (h,) + (0,) * len(shape))
    scratch = []
    operands = list(packed)
    in_specs = [block((blocks, rows, LANES))] * len(packed)
    if got is None:
        shapes = [(size, size)]
    else:
        operands.append(got)
        in_specs.append(block((size, size)))
        shapes = [(cols, size)] * 2
        scratch.append(pltpu.VMEM((PLANES, size, size), jnp.float32))
    outs = pl.pallas_call(
        kernel,
        grid_spec=pltpu.PrefetchScalarGridSpec(
            num_scalar_prefetch=1,
            grid=(part // PLANES,),
            in_specs=in_specs,
            out_specs=[block(shape) for shape in shapes],
            scratch_shapes=scratch,
        ),
        out_shape=[jax.ShapeDtypeStruct((part,) + shape, jnp.bfloat16) for shape in shapes],
        compiler_params=pltpu.CompilerParams(dimension_semantics=("arbitrary",)),
        cost_estimate=pl.CostEstimate(
            flops=6 * part * size * size * LANES,
            bytes_accessed=part * size * (size * 2 + 12 * 3 * LANES),
            transcendentals=0,
        ),
    )(pick, *operands)
    return outs[0] if got is None else outs


def finish_kernel(count, *refs):
    parts = refs[:count]
    normed_ref, gate_w, gate_b, gain, shift, out_w, out_b = refs[count : count + 7]
    out_ref, tri, flat = refs[count + 7 :]
    part, rows = parts[0].shape[0], parts[0].shape[1]
    size = parts[0].shape[2]
    hidden = part * count
    scale = 1.0 / hidden

    def lane_block(step, carry):
        at = pl.multiple_of(step * LANES, LANES)
        for index, ref in enumerate(parts):
            for h in range(part):
                base = (index * part + h) * rows
                tri[base : base + rows, :] = ref[h, :, pl.ds(at, LANES)].astype(jnp.float32)

        for j in range(rows):
            column = tri[pl.ds(j, hidden, stride=rows), :]
            centred = column - jnp.sum(column, axis=0, keepdims=True) * scale
            spread = jnp.sum(centred * centred, axis=0, keepdims=True) * scale
            normed = centred * lax.rsqrt(spread + 1e-05) * gain[...] + shift[...]
            flat[pl.ds(j, LANES, stride=rows), :] = lax.dot_general(
                normed.astype(jnp.bfloat16), out_w[...], TN, preferred_element_type=jnp.float32
            )
        span = LANES

        def write_step(step, carry):
            first = pl.multiple_of(step * span, span)
            channels = normed_ref.shape[2]
            normed = normed_ref[pl.ds(at + first, span), :, :].reshape(span * rows, channels)
            gate = sigmoid(
                jnp.dot(normed, gate_w[...], preferred_element_type=jnp.float32) + gate_b[...]
            )
            base = pl.multiple_of(first * rows, span * rows)
            result = gate * (flat[pl.ds(base, span * rows), :] + out_b[...])
            out_ref[pl.ds(at + first, span), :, :] = result.reshape(span, rows, channels).astype(
                jnp.bfloat16
            )
            return carry

        lax.fori_loop(0, LANES // span, write_step, 0)
        return carry

    lax.fori_loop(0, size // LANES, lane_block, 0)


def finish_local(parts, normed, gate_w, gate_b, gain, shift, out_w, out_b):
    part, cols, size = parts[0].shape
    channels = normed.shape[2]
    hidden = part * len(parts)
    rows = 16
    whole = lambda b: (0, 0)
    positions = cols * size
    return pl.pallas_call(
        functools.partial(finish_kernel, len(parts)),
        grid=(cols // rows,),
        in_specs=[pl.BlockSpec((part, rows, size), lambda b: (0, b, 0))] * len(parts)
        + [
            pl.BlockSpec((size, rows, channels), lambda b: (0, b, 0)),
            pl.BlockSpec(gate_w.shape, whole),
            pl.BlockSpec(gate_b.shape, whole),
            pl.BlockSpec(gain.shape, whole),
            pl.BlockSpec(shift.shape, whole),
            pl.BlockSpec(out_w.shape, whole),
            pl.BlockSpec(out_b.shape, whole),
        ],
        out_specs=pl.BlockSpec((size, rows, channels), lambda b: (0, b, 0)),
        out_shape=jax.ShapeDtypeStruct(normed.shape, jnp.bfloat16),
        scratch_shapes=[
            pltpu.VMEM((hidden * rows, LANES), jnp.float32),
            pltpu.VMEM((LANES * rows, channels), jnp.float32),
        ],
        compiler_params=pltpu.CompilerParams(dimension_semantics=("arbitrary",)),
        cost_estimate=pl.CostEstimate(
            flops=2 * positions * channels * (hidden + channels),
            bytes_accessed=positions * (2 * hidden + 4 * channels),
            transcendentals=positions * channels,
        ),
        name="finish_local",
    )(*parts, normed, gate_w, gate_b, gain, shift, out_w, out_b)


def routes(mesh_shape):
    rows, cols, depths = (mesh_shape[name] for name in AXES)

    def build(target):
        pairs = []
        for r in range(rows):
            for c in range(cols):
                for d in range(depths):
                    to = target(r, c, d)
                    if to is not None:
                        index = lambda at: (at[0] * cols + at[1]) * depths + at[2]
                        pairs.append((index((r, c, d)), index(to)))
        return pairs

    outer = lambda c: c in (0, cols - 1)
    near = lambda c: c ^ 1
    return {
        "inward": build(lambda r, c, d: (r, near(c), d) if outer(c) else None),
        "outward": build(lambda r, c, d: None if outer(c) else (r, near(c), d)),
        "middle": build(lambda r, c, d: None if outer(c) else (r, cols - 1 - c, d)),
        "across": build(lambda r, c, d: None if outer(c) else (rows - 1 - r, c, d)),
        "far": build(lambda r, c, d: (r, c, d ^ 2)),
        "twin": build(lambda r, c, d: (r, c, d ^ 1)),
    }


def folded(
    routing,
    pair,
    ln_gain,
    ln_shift,
    proj_weight,
    proj_bias,
    gate_weight,
    gate_bias,
    out_gain,
    out_shift,
    out_weight,
    out_bias,
):
    depth_count = lax.axis_size("depth")
    row_id, col_id, depth_id = (lax.axis_index(name) for name in AXES)
    channels, cols = pair.shape[2], pair.shape[1]
    hidden = proj_weight.shape[1] // 4
    hid = hidden // depth_count
    pieces = CHUNKS

    def move(value, name):
        return lax.ppermute(value, AXES, routing[name])

    def here(values, axis):
        return lax.dynamic_slice_in_dim(values, depth_id * hid, hid, axis)

    wt = here(proj_weight.T.reshape(4, hidden, channels), 1).reshape(4 * hid, channels)
    bias = here(proj_bias.reshape(4, hidden), 1).reshape(4 * hid, 1)
    normed, left, right = project_local(
        pair, wt, bias, ln_gain[None, :], ln_shift[None, :], pieces
    )

    half_id = col_id // 2
    is_outer = (col_id == 0) | (col_id == lax.axis_size("col") - 1)
    pick = jnp.stack(
        [
            (row_id + half_id != 1).astype(jnp.int32),
            (row_id != half_id).astype(jnp.int32),
            ((col_id % 2) * cols).astype(jnp.int32),
        ]
    )
    own, twin, far, far_twin = [], [], [], []
    for t in range(pieces):
        right_par = move(right[t], "inward")
        left_par = move(left[t], "inward")
        cross_own = move(right[t], "across")
        cross_par = move(right_par, "across")
        packed = (left[t], left_par, right[t], right_par, cross_own, cross_par)
        sent = contract(partial_kernel, pick, packed, None, cols)
        got = move(sent, "middle")
        mine, outers = contract(final_kernel, pick, packed, got, cols)
        mine = jnp.where(is_outer, move(outers, "outward"), mine)
        own.append(mine)
        twin.append(move(mine, "twin"))
        other = move(mine, "far")
        far.append(other)
        far_twin.append(move(other, "twin"))

    order = jnp.concatenate(
        [(depth_id ^ s) * hid + jnp.arange(hid) for s in range(depth_count)]
    )
    return finish_local(
        own + twin + far + far_twin,
        normed,
        gate_weight,
        gate_bias[None, :],
        jnp.broadcast_to(out_gain[order][:, None], (hidden, LANES)),
        jnp.broadcast_to(out_shift[order][:, None], (hidden, LANES)),
        out_weight[order],
        out_bias[None, :],
    )


def solution(mesh):
    placed = (P("row", "col", None), P(), P(), P(), P(), P(), P(), P(), P(), P(), P())
    shape = dict(mesh.shape)

    def spread(body):
        return jax.shard_map(
            body, mesh=mesh, in_specs=placed, out_specs=P("row", "col", None), check_vma=False
        )

    if tuple(shape[name] for name in AXES) != (2, 4, 4):
        return spread(gathered)
    return spread(functools.partial(folded, routes(shape)))
```

```python
import functools

import jax
import jax.numpy as jnp
from jax import lax
from jax.experimental import pallas as pl
from jax.experimental.pallas import tpu as pltpu
from jax.sharding import PartitionSpec as P


AXES = ("row", "col", "depth")
LANES = 128
PAIR = 32
SHARES = (2, 2, 2, 2, 2, 2, 2, 2)
STEPS = 2
ROWS = 32
GATES = 3
LAG = 2
GROUP = 16


def layer_norm(values, gain, shift):
    centre = jnp.mean(values, axis=-1, keepdims=True)
    centred = values - centre
    spread = jnp.mean(centred * centred, axis=-1, keepdims=True)
    return centred * lax.rsqrt(spread + 1e-05) * gain + shift


def project(piece, ln_gain, ln_shift, proj_weight, proj_bias, gate_weight, gate_bias):
    hidden = proj_weight.shape[1] // 4
    channels = piece.shape[2]
    normed = layer_norm(piece.astype(jnp.float32), ln_gain, ln_shift).astype(jnp.bfloat16)
    flat = normed.reshape(-1, channels)
    mixed = jnp.dot(flat, proj_weight, preferred_element_type=jnp.float32) + proj_bias
    left = (jax.nn.sigmoid(mixed[:, :hidden]) * mixed[:, hidden : 2 * hidden]).astype(jnp.bfloat16)
    right = (jax.nn.sigmoid(mixed[:, 2 * hidden : 3 * hidden]) * mixed[:, 3 * hidden :]).astype(
        jnp.bfloat16
    )
    gate = jax.nn.sigmoid(
        jnp.dot(flat, gate_weight, preferred_element_type=jnp.float32) + gate_bias
    )
    shape = (piece.shape[0], piece.shape[1])
    return (
        left.reshape(shape + (hidden,)),
        right.reshape(shape + (hidden,)),
        gate.reshape(shape + (channels,)),
    )


def finish(triangle, gate, out_gain, out_shift, out_weight, out_bias):
    hidden = triangle.shape[2]
    tri_normed = layer_norm(triangle, out_gain, out_shift).astype(jnp.bfloat16)
    projected = (
        jnp.dot(tri_normed.reshape(-1, hidden), out_weight, preferred_element_type=jnp.float32)
        + out_bias
    )
    return (gate * projected.reshape(gate.shape)).astype(jnp.bfloat16)


def gathered(
    pair,
    ln_gain,
    ln_shift,
    proj_weight,
    proj_bias,
    gate_weight,
    gate_bias,
    out_gain,
    out_shift,
    out_weight,
    out_bias,
):
    depth_count = lax.axis_size("depth")
    depth_id = lax.axis_index("depth")
    cols_here = pair.shape[1]
    quarter = cols_here // depth_count
    piece = lax.dynamic_slice_in_dim(pair, depth_id * quarter, quarter, 1)
    left, right, gate = project(
        piece, ln_gain, ln_shift, proj_weight, proj_bias, gate_weight, gate_bias
    )
    left_all = lax.all_gather(left, ("col", "depth"), axis=1, tiled=True)
    right_column = lax.all_gather(right, "row", axis=0, tiled=True)
    needed = lax.all_to_all(right_column, ("col", "depth"), split_axis=0, concat_axis=1, tiled=True)
    triangle = jnp.einsum("ikc,jkc->ijc", left_all, needed, preferred_element_type=jnp.float32)
    finished = finish(triangle, gate, out_gain, out_shift, out_weight, out_bias)
    return lax.all_gather(finished, "depth", axis=1, tiled=True)


def sigmoid(values):
    return 0.5 * jnp.tanh(0.5 * values) + 0.5


NT = (((1,), (1,)), ((), ()))
TN = (((0,), (0,)), ((), ()))


def project_kernel(depth, x_ref, weight_ref, all_bias_ref, gain_ref, shift_ref, normed_ref, *rest):
    outs, (held, turned, wt_ref, bias_ref) = rest[:-4], rest[-4:]
    block, cols = x_ref.shape[0], x_ref.shape[1]
    tail = cols - LANES
    half = block // 2
    rows = block + half
    pitch = rows + 8
    hid = wt_ref.shape[0] // 4
    hidden = weight_ref.shape[1] // 4
    ones = jnp.full((LANES, LANES), 1.0 / LANES, jnp.bfloat16)

    @pl.when(pl.program_id(0) == 0)
    def _():
        turned[...] = weight_ref[...].astype(jnp.float32).T
        for q in range(4):
            at = pl.multiple_of(q * hidden + depth[0] * hid, hid)
            wt_ref[q * hid : (q + 1) * hid, :] = turned[pl.ds(at, hid), :].astype(jnp.bfloat16)
        turned[...] = jnp.broadcast_to(all_bias_ref[...], (LANES, 4 * hidden)).T
        for q in range(4):
            at = pl.multiple_of(q * hidden + depth[0] * hid, hid)
            bias_ref[q * hid : (q + 1) * hid, :] = turned[pl.ds(at, hid), :]

    def tiles(x, first, count):
        flat = x.reshape(count * LANES, LANES)
        centre = jnp.dot(flat, ones, preferred_element_type=jnp.float32)
        centred = flat.astype(jnp.float32) - centre
        spread = jnp.dot(
            (centred * centred).astype(jnp.bfloat16), ones, preferred_element_type=jnp.float32
        )
        normed = (
            centred * lax.rsqrt(spread + 1e-05) * gain_ref[...] + shift_ref[...]
        ).astype(jnp.bfloat16)
        mixed = lax.dot_general(wt_ref[...], normed, NT, preferred_element_type=jnp.float32)
        for t in range(count):
            part = mixed[:, t * LANES : (t + 1) * LANES] + bias_ref[...]
            left = sigmoid(part[:hid]) * part[hid : 2 * hid]
            right = sigmoid(part[2 * hid : 3 * hid]) * part[3 * hid :]
            held[pl.ds(first + t, hid, stride=pitch), :] = left
            held[pl.ds(hid * pitch + first + t, hid, stride=pitch), :] = right
        return normed.reshape(count, LANES, LANES)

    def main(step, carry):
        at = pl.multiple_of(step * GROUP, GROUP)
        normed_ref[pl.ds(at, GROUP), :LANES, :] = tiles(
            x_ref[pl.ds(at, GROUP), :LANES, :], at, GROUP
        )
        return carry

    def leftover(step, carry):
        at = pl.multiple_of(step * GROUP, GROUP)
        x = jnp.concatenate(
            [x_ref[pl.ds(at, GROUP), LANES:, :], x_ref[pl.ds(at + half, GROUP), LANES:, :]], axis=1
        )
        normed = tiles(x, block + at, GROUP)
        normed_ref[pl.ds(at, GROUP), LANES:, :] = normed[:, :tail]
        normed_ref[pl.ds(at + half, GROUP), LANES:, :] = normed[:, tail:]
        return carry

    lax.fori_loop(0, block // GROUP, main, 0, unroll=True)
    lax.fori_loop(0, half // GROUP, leftover, 0)
    first = 0
    for out in outs:
        for h in range(out.shape[0]):
            out[h, 0] = held[first : first + rows, :].astype(jnp.bfloat16)
            first += pitch


def project_local(depth, pair, weight, bias, gain, shift, parts):
    rows_here, cols, channels = pair.shape
    hid = sum(parts)
    blocks = rows_here // PAIR
    packed = PAIR + PAIR // 2
    whole = lambda b, _: (0, 0)
    rowwise = pl.BlockSpec((PAIR, cols, channels), lambda b, _: (b, 0, 0))
    positions = rows_here * cols
    outs = pl.pallas_call(
        project_kernel,
        grid_spec=pltpu.PrefetchScalarGridSpec(
            num_scalar_prefetch=1,
            grid=(blocks,),
            in_specs=[rowwise]
            + [pl.BlockSpec(value.shape, whole) for value in (weight, bias, gain, shift)],
            out_specs=[rowwise]
            + [
                pl.BlockSpec((part, 1, packed, LANES), lambda b, _: (0, b, 0, 0))
                for part in parts + parts
            ],
            scratch_shapes=[
                pltpu.VMEM((2 * hid * (packed + 8), LANES), jnp.float32),
                pltpu.VMEM((weight.shape[1], channels), jnp.float32),
                pltpu.VMEM((4 * hid, channels), jnp.bfloat16),
                pltpu.VMEM((4 * hid, LANES), jnp.float32),
            ],
        ),
        out_shape=[jax.ShapeDtypeStruct(pair.shape, jnp.bfloat16)]
        + [
            jax.ShapeDtypeStruct((part, blocks, packed, LANES), jnp.bfloat16)
            for part in parts + parts
        ],
        compiler_params=pltpu.CompilerParams(dimension_semantics=("arbitrary",)),
        cost_estimate=pl.CostEstimate(
            flops=12 * positions * channels * hid,
            bytes_accessed=positions * (4 * channels + 4 * hid),
            transcendentals=positions * (channels + 2 * hid),
        ),
        name="project_local",
    )(depth, pair, weight, bias, gain, shift)
    return outs[0], outs[1 : 1 + len(parts)], outs[1 + len(parts) :]


def gate_kernel(normed_ref, weight_ref, bias_ref, *refs):
    out_ref = refs[-1]
    block, cols, channels = normed_ref.shape
    span = block // 2
    for first in range(0, block, span):
        flat = normed_ref[first : first + span].reshape(span * cols, channels)
        mixed = jnp.dot(flat, weight_ref[...], preferred_element_type=jnp.float32) + bias_ref[...]
        out_ref[first : first + span] = (
            sigmoid(mixed).astype(jnp.bfloat16).reshape(span, cols, channels)
        )


def gate_local(normed, weight, bias, index, before):
    rows_here, cols, channels = normed.shape
    steps = rows_here // (PAIR * GATES)
    whole = lambda b: (0, 0)
    rowwise = pl.BlockSpec((PAIR, cols, channels), lambda b: (index * steps + b, 0, 0))
    positions = rows_here * cols // GATES
    held = [] if before is None else [before]
    return pl.pallas_call(
        gate_kernel,
        grid=(steps,),
        in_specs=[rowwise, pl.BlockSpec(weight.shape, whole), pl.BlockSpec(bias.shape, whole)]
        + [pl.BlockSpec(memory_space=pl.ANY)] * len(held),
        out_specs=rowwise,
        out_shape=jax.ShapeDtypeStruct(normed.shape, jnp.bfloat16),
        input_output_aliases={3: 0} if held else {},
        compiler_params=pltpu.CompilerParams(dimension_semantics=("arbitrary",)),
        cost_estimate=pl.CostEstimate(
            flops=2 * positions * channels * channels,
            bytes_accessed=4 * positions * channels,
            transcendentals=positions * channels,
        ),
        name="gate_local",
    )(normed, weight, bias, *held)


def operand(own, par):
    blocks = own.shape[0]
    half = PAIR // 2

    def turned(x):
        flat = x.reshape(blocks * half, LANES).astype(jnp.float32)
        return pltpu.roll(flat, LANES // 2, 1).astype(jnp.bfloat16).reshape(x.shape)

    own_rest, par_rest = own[:, PAIR:, :], par[:, PAIR:, :]
    low = lax.broadcasted_iota(jnp.int32, own_rest.shape, 2) < LANES // 2
    first = jnp.where(low, own_rest, turned(par_rest))
    second = jnp.where(low, turned(own_rest), par_rest)
    rest = jnp.concatenate([first[:, None], second[:, None]], axis=1)
    flat = (blocks * PAIR, LANES)
    return jnp.concatenate(
        [own[:, :PAIR, :].reshape(flat), par[:, :PAIR, :].reshape(flat), rest.reshape(flat)],
        axis=1,
    )


def product(here, h, lo, lp, ro, rp, xo, xp):
    own = jnp.where(here, ro[h], xo[h])
    par = jnp.where(here, rp[h], xp[h])
    return lax.dot_general(
        operand(own, par), operand(lo[h], lp[h]), NT, preferred_element_type=jnp.float32
    )


def contract_kernel(sends, ends, pick, *refs):
    total = refs[-1]
    refs = list(refs)
    fresh = [refs.pop(0) for _ in range(6)] if sends else None
    older = [refs.pop(0) for _ in range(7)] if ends else None
    if sends:
        sent_ref = refs.pop(0)
        for h in range(sent_ref.shape[0]):
            sent_ref[h] = product(pick[0] == 0, h, *fresh).astype(jnp.bfloat16)
    if ends:
        mine_ref, outer_ref = refs[0], refs[1]
        got_ref = older[6]
        rows = mine_ref.shape[1]
        mine = pl.multiple_of(pick[2], rows)
        other = pl.multiple_of(rows - pick[2], rows)
        for h in range(mine_ref.shape[0]):
            total[h] = product(pick[1] == 0, h, *older[:6]) + got_ref[h].astype(jnp.float32)
            mine_ref[h] = total[h, pl.ds(mine, rows), :].astype(jnp.bfloat16)
            outer_ref[h] = total[h, pl.ds(other, rows), :].astype(jnp.bfloat16)


def contract(pick, fresh, older, cols):
    size = 2 * cols
    operands, in_specs, out_specs, out_shape = [], [], [], []
    flops, moved, depth = 0, 0, 1

    def block(shape):
        part = shape[0] // STEPS
        return pl.BlockSpec(
            (part,) + shape[1:], lambda h, _: (h,) + (0,) * (len(shape) - 1)
        )

    for values, widths in ((fresh, (size,)), (older, (cols, cols))):
        if values is None:
            continue
        part = values[0].shape[0]
        operands += values
        in_specs += [block(value.shape) for value in values]
        shapes = [(part, width, size) for width in widths]
        out_specs += [block(shape) for shape in shapes]
        out_shape += [jax.ShapeDtypeStruct(shape, jnp.bfloat16) for shape in shapes]
        flops += 6 * part * size * size * LANES
        moved += part * size * (size * 2 + 12 * 3 * LANES)
        depth = max(depth, part // STEPS)
    return pl.pallas_call(
        functools.partial(contract_kernel, fresh is not None, older is not None),
        grid_spec=pltpu.PrefetchScalarGridSpec(
            num_scalar_prefetch=1,
            grid=(STEPS,),
            in_specs=in_specs,
            out_specs=out_specs,
            scratch_shapes=[pltpu.VMEM((depth, size, size), jnp.float32)],
        ),
        out_shape=out_shape,
        compiler_params=pltpu.CompilerParams(dimension_semantics=("arbitrary",)),
        cost_estimate=pl.CostEstimate(flops=flops, bytes_accessed=moved, transcendentals=0),
        name="contract",
    )(pick, *operands)


def finish_kernel(count, groups, depth, *refs):
    parts, refs = refs[:count], refs[count:]
    weights, gains, shifts = (refs[g * groups : (g + 1) * groups] for g in range(3))
    gate_ref, out_b, out_ref, tri, flat = refs[3 * groups :]
    rows = parts[0].shape[1]
    pitch = rows + 8
    size = parts[0].shape[2]
    hidden = tri.shape[0] // pitch
    scale = 1.0 / hidden
    out_w = jnp.concatenate([ref[0] for ref in weights], axis=0)
    stretched = lambda taken: jnp.concatenate(
        [jnp.broadcast_to(ref[0], (hidden // groups, LANES)) for ref in taken], axis=0
    )
    gain = stretched(gains)
    offset = out_b[...] + jnp.sum(
        stretched(shifts) * out_w.astype(jnp.float32), axis=0, keepdims=True
    )

    def lane_block(step, carry):
        at = pl.multiple_of(step * LANES, LANES)
        base = 0
        for ref in parts:
            for h in range(ref.shape[0]):
                tri[base : base + rows, :] = ref[h, :, pl.ds(at, LANES)].astype(jnp.float32)
                base += pitch

        for j in range(rows):
            column = tri[pl.ds(j, hidden, stride=pitch), :]
            centred = column - jnp.sum(column, axis=0, keepdims=True) * scale
            spread = jnp.sum(centred * centred, axis=0, keepdims=True) * scale
            normed = centred * lax.rsqrt(spread + 1e-05) * gain
            flat[pl.ds(j, LANES, stride=pitch), :] = lax.dot_general(
                normed.astype(jnp.bfloat16), out_w, TN, preferred_element_type=jnp.float32
            )
        channels = gate_ref.shape[2]
        update = flat[...].reshape(LANES, pitch, channels)[:, :rows] + offset
        gate = gate_ref[pl.ds(at, LANES), :, :].astype(jnp.float32)
        out_ref[pl.ds(at, LANES), :, :] = (gate * update).astype(jnp.bfloat16)
        return carry

    lax.fori_loop(0, size // LANES, lane_block, 0)


def finish_local(depth, parts, gate, gain, shift, out_w, out_b, groups):
    _, cols, size = parts[0].shape
    channels = gate.shape[2]
    hidden = sum(value.shape[0] for value in parts)
    rows = ROWS
    pitch = rows + 8
    whole = lambda b, _: (0, 0)
    positions = cols * size

    def group(width, s):
        return pl.BlockSpec((1, hidden // groups, width), lambda b, depth: (depth[0] ^ s, 0, 0))

    columns = pl.BlockSpec((size, rows, channels), lambda b, _: (0, b, 0))
    return pl.pallas_call(
        functools.partial(finish_kernel, len(parts), groups),
        grid_spec=pltpu.PrefetchScalarGridSpec(
            num_scalar_prefetch=1,
            grid=(cols // rows,),
            in_specs=[
                pl.BlockSpec((value.shape[0], rows, size), lambda b, _: (0, b, 0))
                for value in parts
            ]
            + [group(channels, s) for s in range(groups)]
            + [group(1, s) for s in range(groups)] * 2
            + [columns]
            + [pl.BlockSpec(out_b.shape, whole)],
            out_specs=columns,
            scratch_shapes=[
                pltpu.VMEM((hidden * pitch, LANES), jnp.float32),
                pltpu.VMEM((LANES * pitch, channels), jnp.float32),
            ],
        ),
        out_shape=jax.ShapeDtypeStruct(gate.shape, jnp.bfloat16),
        compiler_params=pltpu.CompilerParams(dimension_semantics=("arbitrary",)),
        cost_estimate=pl.CostEstimate(
            flops=2 * positions * channels * hidden,
            bytes_accessed=positions * (2 * hidden + 4 * channels),
            transcendentals=positions,
        ),
        name="finish_local",
    )(
        depth,
        *parts,
        *[out_w] * groups,
        *[gain] * groups,
        *[shift] * groups,
        gate,
        out_b,
    )


def routes(mesh_shape):
    rows, cols, depths = (mesh_shape[name] for name in AXES)

    def build(target):
        pairs = []
        for r in range(rows):
            for c in range(cols):
                for d in range(depths):
                    to = target(r, c, d)
                    if to is not None:
                        index = lambda at: (at[0] * cols + at[1]) * depths + at[2]
                        pairs.append((index((r, c, d)), index(to)))
        return pairs

    outer = lambda c: c in (0, cols - 1)
    near = lambda c: c ^ 1
    return {
        "inward": build(lambda r, c, d: (r, near(c), d) if outer(c) else None),
        "outward": build(lambda r, c, d: None if outer(c) else (r, near(c), d)),
        "middle": build(lambda r, c, d: None if outer(c) else (r, cols - 1 - c, d)),
        "across": build(lambda r, c, d: None if outer(c) else (rows - 1 - r, c, d)),
        "far": build(lambda r, c, d: (r, c, d ^ 2)),
        "twin": build(lambda r, c, d: (r, c, d ^ 1)),
    }


def folded(
    routing,
    pair,
    ln_gain,
    ln_shift,
    proj_weight,
    proj_bias,
    gate_weight,
    gate_bias,
    out_gain,
    out_shift,
    out_weight,
    out_bias,
):
    depth_count = lax.axis_size("depth")
    row_id, col_id, depth_id = (lax.axis_index(name) for name in AXES)
    cols = pair.shape[1]
    hid = proj_weight.shape[1] // (4 * depth_count)
    parts = [hid * share // sum(SHARES) for share in SHARES]
    depth = depth_id.astype(jnp.int32)[None]

    def move(value, name):
        return lax.ppermute(value, AXES, routing[name])

    normed, left, right = project_local(
        depth, pair, proj_weight, proj_bias[None], ln_gain[None], ln_shift[None], parts
    )

    half_id = col_id // 2
    is_outer = (col_id == 0) | (col_id == lax.axis_size("col") - 1)
    pick = jnp.stack(
        [
            (row_id + half_id != 1).astype(jnp.int32),
            (row_id != half_id).astype(jnp.int32),
            ((col_id % 2) * cols).astype(jnp.int32),
        ]
    )
    own, twin, far, far_twin = [], [], [], []
    count = len(parts)
    packed, got = {}, {}

    def settle(mine, outers):
        mine = jnp.where(is_outer, move(outers, "outward"), mine)
        own.append(mine)
        twin.append(move(mine, "twin"))
        other = move(mine, "far")
        far.append(other)
        far_twin.append(move(other, "twin"))

    closing = [value.reshape(depth_count, hid, -1) for value in (out_gain, out_shift, out_weight)]
    gate = None
    for g in range(GATES):
        gate = gate_local(normed, gate_weight, gate_bias[None], g, gate)
    for t in range(count):
        right_par = move(right[t], "inward")
        left_par = move(left[t], "inward")
        if t == 2:
            left_par, *closing = lax.optimization_barrier([left_par] + closing)
        cross_own = move(right[t], "across")
        cross_par = move(right_par, "across")
        packed[t] = [left[t], left_par, right[t], right_par, cross_own, cross_par]
        old = t - LAG
        older = packed[old] + [got[old]] if old >= 0 else None
        sent, *done = contract(pick, packed[t], older, cols)
        got[t] = move(sent, "middle")
        if done:
            settle(*done)
    for t in range(max(count - LAG, 0), count):
        done = contract(pick, None, packed[t] + [got[t]], cols)
        settle(*done)

    return finish_local(
        depth,
        own + twin + far + far_twin,
        gate,
        *closing,
        out_bias[None],
        depth_count,
    )


def solution(mesh):
    placed = (P("row", "col", None), P(), P(), P(), P(), P(), P(), P(), P(), P(), P())
    shape = dict(mesh.shape)

    def spread(body):
        return jax.shard_map(
            body, mesh=mesh, in_specs=placed, out_specs=P("row", "col", None), check_vma=False
        )

    if tuple(shape[name] for name in AXES) != (2, 4, 4):
        return spread(gathered)
    return spread(functools.partial(folded, routes(shape)))
```
